32 devices in a mesh: clip: 2 (over core), ha: 4 (over y, x), wa: 4 (over z).
Axes of the slice: x: 2, y: 2, z: 4, core: 2. Of those that a mesh axis runs over, the one named last changes fastest.
Arguments:
- frames: bfloat16 [8, 96, 128, 128], P('clip', 'ha', 'wa'), parts along dimension 0, may hold values from -60 to 60, as said below
- caches: bfloat16 [4, 4, 96, 128, 128], P('clip', None, 'ha', 'wa'), parts along dimension 0, may hold values from -4 to 4
- conv_weights: bfloat16 [4, 3, 3, 3, 128, 128], replicated, may hold values from -0.109375 to 0.109375
- conv_bias: float32 [4, 128], replicated, may hold values from -3 to 3
- norm_gain: float32 [4, 128], replicated, may hold values from 0.25 to 1.75
- norm_shift: float32 [4, 128], replicated, may hold values from -3 to 3
Outputs:
- encoded: bfloat16 [8, 96, 128, 128], P('clip', 'ha', 'wa'), parts along dimension 0
- new_caches: bfloat16 [4, 4, 96, 128, 128], P('clip', None, 'ha', 'wa'), parts along dimension 0
The draws below stay inside these ranges and needn't reach their ends.
There are 2 independent parts, one for each index of `clip`. The reference program is written for one: setup_inputs(seed, part) draws one part's arguments, and reference() takes and returns one part's arrays. A program takes and returns all parts, laid end to end along the dimension named above; an argument that names none is the same for every part. Nothing has to cross between parts.
Inputs may be any that keep to these rules, and one draw needn't show every extreme that they name: `frames`: real-valued features.
All inputs are finite; a program needn't handle non-finite values.
Results may differ from the reference program's by a relative error of at most 0.005.
Values may be sent and summed in bfloat16 or wider, within the bound.
A program may use at most 64 MiB of HBM per device.

```python
import jax
import jax.numpy as jnp
from jax import lax

C = 128
GROUPS = 32
FR = 4
BLOCKS = 2
CACHE = 2
CONVS = 4
H = 96
W = 128


def draw_frames(key, part):
    streams = jax.random.split(jax.random.fold_in(key, 11), 3)
    row_pos = jnp.arange(H, dtype=jnp.float32) / (H - 1)
    col_pos = jnp.arange(W, dtype=jnp.float32) / (W - 1)
    trend = jnp.log(0.5) + jnp.log(3.0) * 0.5 * (row_pos[:, None] + col_pos[None, :])
    cell_level = jax.random.uniform(streams[0], (FR, H, W, 1), jnp.float32, -1.15, 1.15)
    channel_level = jnp.exp(jax.random.uniform(streams[1], (C,), jnp.float32, -1.15, 1.15))
    noise = jnp.clip(jax.random.normal(streams[2], (FR, H, W, C), jnp.float32), -3.0, 3.0)
    values = jnp.exp(trend[None, :, :, None] + cell_level) * channel_level * noise
    return values.astype(jnp.bfloat16)


def block_scale(stream_key, dims, pieces, low, high):
    factor_of = 1.0
    for dim, shards_of in pieces:
        heights = jax.random.uniform(jax.random.fold_in(jax.random.fold_in(stream_key, 6), dim), (shards_of,), jnp.float32, low / len(pieces), high / len(pieces))
        factor_of = factor_of * jnp.repeat(jnp.exp(heights), dims[dim] // shards_of).reshape((-1,) + (1,) * (len(dims) - 1 - dim))
    return factor_of


def gaussian(key, shape, spread, most, cuts=(), held_as=jnp.bfloat16):
    values = spread * jax.random.normal(key, shape, jnp.float32)
    if cuts:
        values = values * block_scale(key, shape, cuts, -0.22, 0.18)
    return jnp.clip(values, -most, most).astype(held_as)


def setup_inputs(seed: int = 0, part: int = 0) -> dict:
    keys = jax.random.split(jax.random.key(seed), 7)
    part_keys = jax.random.split(jax.random.fold_in(keys[6], part), 7)
    frames = draw_frames(jax.random.fold_in(jax.random.fold_in(keys[6], part), 71), part)
    caches = gaussian(part_keys[1], (CACHE, CONVS, H, W, C), 1.0, 4.0, ((2, 4), (3, 4)))
    conv_weights = gaussian(keys[2], (CONVS, 3, 3, 3, C, C), (27 * C) ** -0.5, 0.109375)
    conv_bias = gaussian(keys[3], (CONVS, C), 0.5, 3.0, (), jnp.float32)
    norm_gain = jnp.clip(1.0 + 0.15 * jax.random.normal(keys[4], (CONVS, C), jnp.float32), 0.25, 1.75)
    norm_shift = gaussian(keys[5], (CONVS, C), 0.5, 3.0, (), jnp.float32)
    return {"frames": frames, "caches": caches, "conv_weights": conv_weights, "conv_bias": conv_bias, "norm_gain": norm_gain, "norm_shift": norm_shift}


EPSILON = 1e-06

def group_norm(values, gain_row, shift_row):
    grouped = values.reshape(values.shape[0], values.shape[1], values.shape[2], GROUPS, -1)
    group_mean = lax.optimization_barrier(jnp.mean(grouped, axis=(0, 1, 2, 4), keepdims=True))
    centered = grouped - group_mean
    variance = lax.optimization_barrier(jnp.mean(centered * centered, axis=(0, 1, 2, 4), keepdims=True))
    normed = centered / jnp.sqrt(variance + EPSILON)
    return normed.reshape(values.shape) * gain_row + shift_row

def causal_conv(activation, history, kernel, bias_row):
    joined = jnp.concatenate([history, activation], axis=0).astype(jnp.float32)
    padded = jnp.pad(joined, ((0, 0), (1, 1), (1, 1), (0, 0)))
    result = lax.conv_general_dilated(padded[None], kernel.astype(jnp.float32), (1, 1, 1), 'VALID', dimension_numbers=('NDHWC', 'DHWIO', 'NDHWC'), precision=lax.Precision.HIGHEST)
    return result[0] + bias_row

def reference(frames, caches, conv_weights, conv_bias, norm_gain, norm_shift):
    block_input = frames
    saved = []
    for block_index in range(BLOCKS):
        first_conv = 2 * block_index
        second_conv = first_conv + 1
        first_act = jax.nn.silu(group_norm(block_input.astype(jnp.float32), norm_gain[first_conv], norm_shift[first_conv])).astype(jnp.bfloat16)
        saved.append(first_act[FR - CACHE:])
        middle = causal_conv(first_act, caches[:, first_conv], conv_weights[first_conv], conv_bias[first_conv])
        second_act = jax.nn.silu(group_norm(middle, norm_gain[second_conv], norm_shift[second_conv])).astype(jnp.bfloat16)
        saved.append(second_act[FR - CACHE:])
        branch = causal_conv(second_act, caches[:, second_conv], conv_weights[second_conv], conv_bias[second_conv])
        block_input = (block_input.astype(jnp.float32) + branch).astype(jnp.bfloat16)
    return (block_input, jnp.stack(saved, axis=1))
```

```python
import functools

import jax
import jax.numpy as jnp
from jax import lax
from jax.experimental import pallas as pl
from jax.experimental.pallas import tpu as pltpu
from jax.sharding import PartitionSpec as P

GROUPS = 32
EPSILON = 1e-06
MESH = pl.DeviceIdType.MESH
F32 = jnp.float32
BF16 = jnp.bfloat16
ROW_BLOCK = 8
DIRECTIONS = [(dy, dx) for dy in (-1, 0, 1) for dx in (-1, 0, 1) if (dy, dx) != (0, 0)]


def kernel(dims, *refs):
    (frames, caches, weights, bias, gain, shift, encoded, kept,
     x, cb, v, vc, a, t, acc, y,
     s_out, s_in,
     lc_out, lk_out, lr_in, lc_in, lk_in,
     cc_out, ck_out, cr_in, cc_in, ck_in,
     load_sem, weight_sem, kept_sem, out_sem,
     stat_send, stat_recv, halo_send, halo_recv) = refs
    nh, nw, fr, cf, convs, h, w, c = dims
    pitch = w + 8
    peers = nh * nw
    cell_count = fr * h * w * peers * (c // GROUPS)
    clip, ha, wa = lax.axis_index("clip"), lax.axis_index("ha"), lax.axis_index("wa")
    me = ha * nw + wa
    others = [
        (lax.rem(ha + i, nh), lax.rem(wa + j, nw))
        for i in range(nh)
        for j in range(nw)
        if (i, j) != (0, 0)
    ]
    barrier = pltpu.get_barrier_semaphore()
    for ph, pw in others:
        pl.semaphore_signal(barrier, inc=1, device_id=(clip, ph, pw), device_id_type=MESH)

    load_x = pltpu.make_async_copy(frames, x, load_sem.at[0])
    load_x.start()
    load_c = pltpu.make_async_copy(caches, cb, load_sem.at[1])
    load_c.start()

    def weight_copies(k):
        copies = []
        for dt in range(3):
            for half in range(2):
                copies.append(
                    pltpu.make_async_copy(
                        weights.at[k, dt],
                        t.at[k, dt + half, :, :, pl.ds(half * c, c)],
                        weight_sem.at[k, dt * 2 + half],
                    )
                )
        return copies

    for k in range(convs):
        for copy in weight_copies(k):
            copy.start()

    def zero_weights(k, carry):
        t[k, 3, :, :, 0:c] = jnp.zeros((3, 3 * c, c), BF16)
        t[k, 0, :, :, c : 2 * c] = jnp.zeros((3, 3 * c, c), BF16)
        return carry

    lax.fori_loop(0, convs, zero_weights, 0)

    def exists(dy, dx):
        conds = []
        if dy:
            conds.append(ha > 0 if dy < 0 else ha < nh - 1)
        if dx:
            conds.append(wa > 0 if dx < 0 else wa < nw - 1)
        return conds[0] if len(conds) == 1 else jnp.logical_and(*conds)

    def halo_copy(live, k, dy, dx, towards):
        e = k if live else convs + k
        field = v if live else vc.at[k]
        rows_in = lr_in if live else cr_in
        cols_out, cols_in = (lc_out, lc_in) if live else (cc_out, cc_in)
        ends_out, ends_in = (lk_out, lk_in) if live else (ck_out, ck_in)
        if dx == 0:
            src = field.at[:, pl.ds(0 if dy < 0 else (h - 1) * w, w), :]
            dst = rows_in.at[k, int(dy < 0)]
        elif dy == 0:
            src = cols_out.at[k, int(dx > 0)]
            dst = cols_in.at[k, int(dx < 0)]
        else:
            index = int(dy > 0) * 2 + int(dx > 0)
            src = ends_out.at[k, index]
            dst = ends_in.at[k, 3 - index]
        d = DIRECTIONS.index((dy, dx))
        back = DIRECTIONS.index((-dy, -dx))
        return pltpu.make_async_remote_copy(
            src_ref=src,
            dst_ref=dst,
            send_sem=halo_send.at[e, d],
            recv_sem=halo_recv.at[e, back],
            device_id=(clip, ha + dy * towards, wa + dx * towards),
            device_id_type=MESH,
        )

    def pack_edges(live, k):
        field = v if live else vc.at[k]
        cols_out = lc_out if live else cc_out
        ends_out = lk_out if live else ck_out
        for f in range(fr if live else cf):
            for side in range(2):
                first = side * (w - 1)
                cols_out[k, side, f] = field[f, pl.ds(first, h, stride=w), :]
                for low in range(2):
                    row = low * (h - 1) * w + first
                    ends_out[k, low * 2 + side, f] = field[f, row : row + 1, :]

    def send_halo(live, k):
        pack_edges(live, k)
        for dy, dx in DIRECTIONS:

            @pl.when(exists(dy, dx))
            def _():
                halo_copy(live, k, dy, dx, 1).start()

    def wait_halo(live, k):
        for dy, dx in DIRECTIONS:

            @pl.when(exists(dy, dx))
            def _():
                halo_copy(live, k, -dy, -dx, -1).wait_recv()

    def wait_sent(live, k):
        for dy, dx in DIRECTIONS:

            @pl.when(exists(dy, dx))
            def _():
                halo_copy(live, k, dy, dx, 1).wait_send()

    def stat_copy(k, number, sender):
        ph, pw = others[number]
        return pltpu.make_async_remote_copy(
            src_ref=s_out.at[k],
            dst_ref=s_in.at[k, sender],
            send_sem=stat_send.at[k, number],
            recv_sem=stat_recv.at[k, sender],
            device_id=(clip, ph, pw),
            device_id_type=MESH,
        )

    def send_stats(k, sums, squares):
        both = jnp.concatenate(
            [jnp.sum(sums, axis=0, keepdims=True), jnp.sum(squares, axis=0, keepdims=True)], axis=0
        )
        s_out[k] = both
        s_in[k, me] = both
        for number in range(peers - 1):
            stat_copy(k, number, me).start()

    def wait_stats(k):
        for number, (ph, pw) in enumerate(others):
            stat_copy(k, number, ph * nw + pw).wait_recv()
        total = s_in[k, 0]
        for i in range(1, peers):
            total = total + s_in[k, i]
        total = jnp.concatenate([total, jnp.zeros((6, c), F32)], axis=0)
        lane = lax.broadcasted_iota(jnp.int32, (8, c), 1)
        step = 1
        while step < c // GROUPS:
            total = total + jnp.where(
                lax.rem(lane, 2 * step) < step,
                pltpu.roll(total, c - step, 1),
                pltpu.roll(total, step, 1),
            )
            step *= 2
        mean = total[0:1] / cell_count
        variance = total[1:2] / cell_count - mean * mean
        multiplier = lax.rsqrt(variance + EPSILON) * gain[k : k + 1, :]
        offset = shift[k : k + 1, :] - mean * multiplier
        return multiplier, offset

    def silu(values):
        half = 0.5 * values
        return half + half * jnp.tanh(half)

    def build(par, f, row_of, rows, cols, ends):
        for r in range(h + 2):
            cells = rows[0]() if r == 0 else rows[1]() if r == h + 1 else row_of(r - 1)
            a[par, f, r, :, c : 2 * c] = cells.astype(BF16)
            y[r * pitch + 1 : r * pitch + 1 + w, :] = cells
        for side in range(2):
            edge = side * (w + 1)
            y[pl.ds(pitch + edge, h, stride=pitch), :] = cols[side]()
            for low in range(2):
                at = low * (h + 1) * pitch + edge
                y[at : at + 1, :] = ends[low * 2 + side]()
        for r in range(h + 2):
            for dw in (0, 2):
                at = r * pitch + dw
                a[par, f, r, :, dw * c : (dw + 1) * c] = y[at : at + w, :].astype(BF16)

    def masked(dy, dx, values):
        return jnp.where(exists(dy, dx), values, 0.0)

    SIDE = (-1, 1)

    def build_cached(k):
        par = k % 2

        def body(f, carry):
            build(
                par,
                f,
                lambda r: vc[k, f, r * w : (r + 1) * w, :],
                [lambda i=i: masked(SIDE[i], 0, cr_in[k, i, f]) for i in range(2)],
                [lambda i=i: masked(0, SIDE[i], cc_in[k, i, f]) for i in range(2)],
                [lambda i=i: masked(SIDE[i // 2], SIDE[i % 2], ck_in[k, i, f]) for i in range(4)],
            )
            return carry

        lax.fori_loop(0, cf, body, 0)

    def build_live(k, multiplier, offset):
        par = k % 2

        def act(values):
            return silu(values * multiplier + offset)

        def body(f, carry):
            build(
                par,
                cf + f,
                lambda r: act(v[f, r * w : (r + 1) * w, :]),
                [lambda i=i: masked(SIDE[i], 0, act(lr_in[k, i, f])) for i in range(2)],
                [lambda i=i: masked(0, SIDE[i], act(lc_in[k, i, f])) for i in range(2)],
                [
                    lambda i=i: masked(SIDE[i // 2], SIDE[i % 2], act(lk_in[k, i, f]))
                    for i in range(4)
                ],
            )
            return carry

        lax.fori_loop(0, fr, body, 0)

    def product(k, first, low, high, block):
        par = k % 2
        pieces = []
        for f in range(low, high):
            for dh in range(3):
                piece = a[par, first + f, pl.ds(block * ROW_BLOCK + dh, ROW_BLOCK)]
                pieces.append(piece.reshape(ROW_BLOCK * w, 3 * c))
        left = jnp.concatenate(pieces, axis=1)
        right = t[k, low:high].reshape((high - low) * 9 * c, 2 * c)
        return jnp.dot(left, right, preferred_element_type=F32)

    blocks = h // ROW_BLOCK
    cells = ROW_BLOCK * w

    def conv_cached(k):
        def body(block, carry):
            acc[pl.ds(pl.multiple_of(block * cells, cells), cells), :] = product(k, 0, 0, cf, block)
            return carry

        lax.fori_loop(0, blocks, body, 0)

    def conv_live(k):
        bias_row = bias[k : k + 1, :]
        zero = jnp.zeros((8, c), F32)
        carry = (zero, zero)
        for pair in range(fr // 2):

            def body(block, carry, pair=pair):
                sums, squares = carry
                span = pl.ds(pl.multiple_of(block * cells, cells), cells)
                if pair == 0:
                    both = product(k, 0, cf, cf + 2, block) + acc[span, :]
                else:
                    both = product(k, 2 * pair, 0, 4, block)
                for half in range(2):
                    f = 2 * pair + half
                    result = both[:, half * c : (half + 1) * c] + bias_row
                    if k % 2:
                        rounded = (x[f, span, :].astype(F32) + result).astype(BF16)
                        x[f, span, :] = rounded
                        result = rounded.astype(F32)
                    if k < convs - 1:
                        v[f, span, :] = result
                        slabs = result.reshape(cells // 8, 8, c)
                        sums = sums + jnp.sum(slabs, axis=0)
                        squares = squares + jnp.sum(slabs * slabs, axis=0)
                return sums, squares

            carry = lax.fori_loop(0, blocks, body, carry)
            if k == convs - 1:
                out_copy(pair).start()
        return carry

    def out_copy(pair):
        span = pl.ds(2 * pair, 2)
        return pltpu.make_async_copy(x.at[span], encoded.at[span], out_sem.at[pair])

    def kept_copy(k):
        return pltpu.make_async_copy(
            a.at[k % 2, pl.ds(fr, cf), pl.ds(1, h), :, pl.ds(c, c)], kept.at[:, k], kept_sem.at[k]
        )

    load_x.wait()

    def widen(f, carry):
        sums, squares = carry
        values = x[f].astype(F32)
        v[f] = values
        slabs = values.reshape(h * w // 8, 8, c)
        return sums + jnp.sum(slabs, axis=0), squares + jnp.sum(slabs * slabs, axis=0)

    zero = jnp.zeros((8, c), F32)
    carry = lax.fori_loop(0, fr, widen, (zero, zero))
    pl.semaphore_wait(barrier, peers - 1)
    send_stats(0, *carry)
    send_halo(True, 0)
    load_c.wait()
    for k in range(convs):

        def widen_cache(f, carry, k=k):
            vc[k, f] = cb[f, k].astype(F32)
            return carry

        lax.fori_loop(0, cf, widen_cache, 0)
        send_halo(False, k)

    for k in range(convs):
        if k >= 2:
            kept_copy(k - 2).wait()
        wait_halo(False, k)
        build_cached(k)
        for copy in weight_copies(k):
            copy.wait()
        conv_cached(k)
        multiplier, offset = wait_stats(k)
        wait_halo(True, k)
        build_live(k, multiplier, offset)
        kept_copy(k).start()
        wait_sent(True, k)
        carry = conv_live(k)
        if k < convs - 1:
            send_stats(k + 1, *carry)
            send_halo(True, k + 1)

    for k in range(convs):
        wait_sent(False, k)
        for number in range(peers - 1):
            stat_copy(k, number, me).wait_send()
    for k in range(max(convs - 2, 0), convs):
        kept_copy(k).wait()
    for pair in range(fr // 2):
        out_copy(pair).wait()


def local(nh, nw, frames, caches, conv_weights, conv_bias, norm_gain, norm_shift):
    fr, h, w, c = frames.shape
    cf, convs = caches.shape[:2]
    dims = (nh, nw, fr, cf, convs, h, w, c)
    peers = nh * nw
    vmem = pltpu.VMEM
    dma = pltpu.SemaphoreType.DMA
    scratch = [
        vmem((fr, h * w, c), BF16),
        vmem((cf, convs, h * w, c), BF16),
        vmem((fr, h * w, c), F32),
        vmem((convs, cf, h * w, c), F32),
        vmem((2, fr + cf, h + 2, w, 3 * c), BF16),
        vmem((convs, 4, 3, 3 * c, 2 * c), BF16),
        vmem((h * w, 2 * c), F32),
        vmem(((h + 2) * (w + 8), c), F32),
        vmem((convs, 2, c), F32),
        vmem((convs, peers, 2, c), F32),
    ]
    for nf, sent in ((fr, True), (cf, True)):
        scratch += [
            vmem((convs, 2, nf, h, c), F32),
            vmem((convs, 4, nf, 1, c), F32),
            vmem((convs, 2, nf, w, c), F32),
            vmem((convs, 2, nf, h, c), F32),
            vmem((convs, 4, nf, 1, c), F32),
        ]
    scratch += [
        dma((2,)),
        dma((convs, 6)),
        dma((convs,)),
        dma((fr // 2,)),
        dma((convs, peers - 1)),
        dma((convs, peers)),
        dma((2 * convs, 8)),
        dma((2 * convs, 8)),
    ]
    anywhere = pl.BlockSpec(memory_space=pl.ANY)
    inside = pl.BlockSpec(memory_space=pltpu.VMEM)
    encoded, kept = pl.pallas_call(
        functools.partial(kernel, dims),
        out_shape=(
            jax.ShapeDtypeStruct((fr, h * w, c), BF16),
            jax.ShapeDtypeStruct(caches.shape, BF16),
        ),
        in_specs=[anywhere] * 3 + [inside] * 3,
        out_specs=(anywhere, anywhere),
        scratch_shapes=scratch,
        compiler_params=pltpu.CompilerParams(
            collective_id=0, has_side_effects=True, vmem_limit_bytes=56 * 1024 * 1024
        ),
    )(
        frames.reshape(fr, h * w, c),
        caches.reshape(cf, convs, h * w, c),
        conv_weights.reshape(convs, 3, 3, 3 * c, c),
        conv_bias,
        norm_gain,
        norm_shift,
    )
    return encoded.reshape(frames.shape), kept


def solution(mesh):
    return jax.shard_map(
        functools.partial(local, mesh.shape["ha"], mesh.shape["wa"]),
        mesh=mesh,
        in_specs=(
            P("clip", "ha", "wa", None),
            P("clip", None, "ha", "wa", None),
            P(),
            P(),
            P(),
            P(),
        ),
        out_specs=(P("clip", "ha", "wa", None), P("clip", None, "ha", "wa", None)),
        check_vma=False,
    )
```

```python
import functools

import jax
import jax.numpy as jnp
from jax import lax
from jax.experimental import pallas as pl
from jax.experimental.pallas import tpu as pltpu
from jax.sharding import PartitionSpec as P

GROUPS = 32
EPSILON = 1e-06
MESH = pl.DeviceIdType.MESH
F32 = jnp.float32
BF16 = jnp.bfloat16
ROW_BLOCK = 12
DIRECTIONS = [(dy, dx) for dy in (-1, 0, 1) for dx in (-1, 0, 1) if (dy, dx) != (0, 0)]


def kernel(dims, *refs):
    (frames, caches, weights, bias, gain, shift, encoded, kept,
     x, cb, v, vc, a, t, acc, y,
     s_out, s_in,
     lr_out, lc_out, lk_out, lr_in, lc_in, lk_in,
     cr_out, cc_out, ck_out, cr_in, cc_in, ck_in,
     load_sem, weight_sem, kept_sem, out_sem,
     stat_send, stat_recv, halo_send, halo_recv) = refs
    nh, nw, fr, cf, convs, h, w, c = dims
    pitch = w + 8
    peers = nh * nw
    cell_count = fr * h * w * peers * (c // GROUPS)
    clip, ha, wa = lax.axis_index("clip"), lax.axis_index("ha"), lax.axis_index("wa")
    me = ha * nw + wa
    others = [
        (lax.rem(ha + i, nh), lax.rem(wa + j, nw))
        for i in range(nh)
        for j in range(nw)
        if (i, j) != (0, 0)
    ]
    barrier = pltpu.get_barrier_semaphore()
    for ph, pw in others:
        pl.semaphore_signal(barrier, inc=1, device_id=(clip, ph, pw), device_id_type=MESH)

    load_x = pltpu.make_async_copy(frames, x, load_sem.at[0])
    load_x.start()
    load_c = pltpu.make_async_copy(caches, cb, load_sem.at[1])
    load_c.start()

    def weight_copies(k):
        copies = []
        for dt in range(3):
            for half in range(2):
                copies.append(
                    pltpu.make_async_copy(
                        weights.at[k, dt],
                        t.at[k, dt + half, :, :, pl.ds(half * c, c)],
                        weight_sem.at[k, dt * 2 + half],
                    )
                )
        return copies

    for copy in weight_copies(0):
        copy.start()

    def zero_weights(k, carry):
        t[k, 3, :, :, 0:c] = jnp.zeros((3, 3 * c, c), BF16)
        t[k, 0, :, :, c : 2 * c] = jnp.zeros((3, 3 * c, c), BF16)
        return carry

    lax.fori_loop(0, convs, zero_weights, 0)

    def exists(dy, dx):
        conds = []
        if dy:
            conds.append(ha > 0 if dy < 0 else ha < nh - 1)
        if dx:
            conds.append(wa > 0 if dx < 0 else wa < nw - 1)
        return conds[0] if len(conds) == 1 else jnp.logical_and(*conds)

    parts = fr // 2

    def halo_copy(live, k, part, dy, dx, towards):
        e = k * parts + part if live else convs * parts + k
        span = pl.ds(2 * part, 2) if live else pl.ds(0, cf)
        rows_out, rows_in = (lr_out, lr_in) if live else (cr_out, cr_in)
        cols_out, cols_in = (lc_out, lc_in) if live else (cc_out, cc_in)
        ends_out, ends_in = (lk_out, lk_in) if live else (ck_out, ck_in)
        if dx == 0:
            src = rows_out.at[k, int(dy > 0), span]
            dst = rows_in.at[k, int(dy < 0), span]
        elif dy == 0:
            src = cols_out.at[k, int(dx > 0), span]
            dst = cols_in.at[k, int(dx < 0), span]
        else:
            index = int(dy > 0) * 2 + int(dx > 0)
            src = ends_out.at[k, index, span]
            dst = ends_in.at[k, 3 - index, span]
        d = DIRECTIONS.index((dy, dx))
        back = DIRECTIONS.index((-dy, -dx))
        return pltpu.make_async_remote_copy(
            src_ref=src,
            dst_ref=dst,
            send_sem=halo_send.at[e, d],
            recv_sem=halo_recv.at[e, back],
            device_id=(clip, ha + dy * towards, wa + dx * towards),
            device_id_type=MESH,
        )

    def pack_edges(live, k, part):
        field = v if live else vc.at[k]
        rows_out = lr_out if live else cr_out
        cols_out = lc_out if live else cc_out
        ends_out = lk_out if live else ck_out
        for f in range(2 * part, 2 * part + 2) if live else range(cf):
            for side in range(2):
                first = side * (w - 1)
                top = side * (h - 1) * w
                rows_out[k, side, f] = field[f, top : top + w, :].astype(BF16)
                cols_out[k, side, f] = field[f, pl.ds(first, h, stride=w), :].astype(BF16)
                for low in range(2):
                    row = low * (h - 1) * w + first
                    ends_out[k, low * 2 + side, f] = field[f, row : row + 1, :]

    def send_halo(live, k, part):
        pack_edges(live, k, part)
        for dy, dx in DIRECTIONS:

            @pl.when(exists(dy, dx))
            def _():
                halo_copy(live, k, part, dy, dx, 1).start()

    def wait_halo(live, k):
        for dy, dx in DIRECTIONS:

            @pl.when(exists(dy, dx))
            def _():
                for part in range(parts if live else 1):
                    halo_copy(live, k, part, -dy, -dx, -1).wait_recv()

    def wait_sent(live, k):
        for dy, dx in DIRECTIONS:

            @pl.when(exists(dy, dx))
            def _():
                for part in range(parts if live else 1):
                    halo_copy(live, k, part, dy, dx, 1).wait_send()

    def stat_copy(k, number, sender):
        ph, pw = others[number]
        return pltpu.make_async_remote_copy(
            src_ref=s_out.at[k],
            dst_ref=s_in.at[k, sender],
            send_sem=stat_send.at[k, number],
            recv_sem=stat_recv.at[k, sender],
            device_id=(clip, ph, pw),
            device_id_type=MESH,
        )

    def send_stats(k, sums, squares):
        both = jnp.concatenate(
            [jnp.sum(sums, axis=0, keepdims=True), jnp.sum(squares, axis=0, keepdims=True)], axis=0
        )
        s_out[k] = both
        s_in[k, me] = both
        for number in range(peers - 1):
            stat_copy(k, number, me).start()

    def wait_stats(k):
        for number, (ph, pw) in enumerate(others):
            stat_copy(k, number, ph * nw + pw).wait_recv()
        total = s_in[k, 0]
        for i in range(1, peers):
            total = total + s_in[k, i]
        total = jnp.concatenate([total, jnp.zeros((6, c), F32)], axis=0)
        lane = lax.broadcasted_iota(jnp.int32, (8, c), 1)
        step = 1
        while step < c // GROUPS:
            total = total + jnp.where(
                lax.rem(lane, 2 * step) < step,
                pltpu.roll(total, c - step, 1),
                pltpu.roll(total, step, 1),
            )
            step *= 2
        mean = total[0:1] / cell_count
        variance = total[1:2] / cell_count - mean * mean
        multiplier = lax.rsqrt(variance + EPSILON) * gain[k : k + 1, :]
        offset = shift[k : k + 1, :] - mean * multiplier
        return multiplier, offset

    def silu(values):
        half = 0.5 * values
        return half + half * jnp.tanh(half)

    def build(par, f, row_of, rows, cols, ends):
        for r in range(h + 2):
            cells = rows[0]() if r == 0 else rows[1]() if r == h + 1 else row_of(r - 1)
            a[par, f, r, :, c : 2 * c] = cells.astype(BF16)
            y[r * pitch + 1 : r * pitch + 1 + w, :] = cells
        for side in range(2):
            edge = side * (w + 1)
            y[pl.ds(pitch + edge, h, stride=pitch), :] = cols[side]()
            for low in range(2):
                at = low * (h + 1) * pitch + edge
                y[at : at + 1, :] = ends[low * 2 + side]()
        for r in range(h + 2):
            for dw in (0, 2):
                at = r * pitch + dw
                a[par, f, r, :, dw * c : (dw + 1) * c] = y[at : at + w, :].astype(BF16)

    def masked(dy, dx, values):
        return jnp.where(exists(dy, dx), values, 0.0)

    SIDE = (-1, 1)

    def build_cached(k):
        par = k % 2

        def body(f, carry):
            build(
                par,
                f,
                lambda r: vc[k, f, r * w : (r + 1) * w, :],
                [lambda i=i: masked(SIDE[i], 0, cr_in[k, i, f].astype(F32)) for i in range(2)],
                [lambda i=i: masked(0, SIDE[i], cc_in[k, i, f].astype(F32)) for i in range(2)],
                [lambda i=i: masked(SIDE[i // 2], SIDE[i % 2], ck_in[k, i, f]) for i in range(4)],
            )
            return carry

        lax.fori_loop(0, cf, body, 0)

    def build_live(k, multiplier, offset):
        par = k % 2

        def act(values):
            return silu(values * multiplier + offset)

        def body(f, carry):
            build(
                par,
                cf + f,
                lambda r: act(v[f, r * w : (r + 1) * w, :]),
                [lambda i=i: masked(SIDE[i], 0, act(lr_in[k, i, f].astype(F32))) for i in range(2)],
                [lambda i=i: masked(0, SIDE[i], act(lc_in[k, i, f].astype(F32))) for i in range(2)],
                [
                    lambda i=i: masked(SIDE[i // 2], SIDE[i % 2], act(lk_in[k, i, f]))
                    for i in range(4)
                ],
            )
            return carry

        lax.fori_loop(0, fr, body, 0)

    def product(k, first, low, high, block):
        par = k % 2
        pieces = []
        for f in range(low, high):
            for dh in range(3):
                piece = a[par, first + f, pl.ds(block * ROW_BLOCK + dh, ROW_BLOCK)]
                pieces.append(piece.reshape(ROW_BLOCK * w, 3 * c))
        left = jnp.concatenate(pieces, axis=1)
        right = t[k, low:high].reshape((high - low) * 9 * c, 2 * c)
        return jnp.dot(left, right, preferred_element_type=F32)

    blocks = h // ROW_BLOCK
    cells = ROW_BLOCK * w

    def conv_cached(k):
        def body(block, carry):
            acc[pl.ds(pl.multiple_of(block * cells, cells), cells), :] = product(k, 0, 0, cf, block)
            return carry

        lax.fori_loop(0, blocks, body, 0)

    def conv_live(k):
        bias_row = bias[k : k + 1, :]
        zero = jnp.zeros((8, c), F32)
        carry = (zero, zero)
        for pair in range(fr // 2):

            def body(block, carry, pair=pair):
                sums, squares = carry
                span = pl.ds(pl.multiple_of(block * cells, cells), cells)
                if pair == 0:
                    both = product(k, 0, cf, cf + 2, block) + acc[span, :]
                else:
                    both = product(k, 2 * pair, 0, 4, block)
                for half in range(2):
                    f = 2 * pair + half
                    result = both[:, half * c : (half + 1) * c] + bias_row
                    if k % 2:
                        rounded = (x[f, span, :].astype(F32) + result).astype(BF16)
                        x[f, span, :] = rounded
                        result = rounded.astype(F32)
                    if k < convs - 1:
                        v[f, span, :] = result
                        slabs = result.reshape(cells // 8, 8, c)
                        sums = sums + jnp.sum(slabs, axis=0)
                        squares = squares + jnp.sum(slabs * slabs, axis=0)
                return sums, squares

            carry = lax.fori_loop(0, blocks, body, carry)
            if k == convs - 1:
                out_copy(pair).start()
            elif pair < parts - 1:
                send_halo(True, k + 1, pair)
        return carry

    def out_copy(pair):
        span = pl.ds(2 * pair, 2)
        return pltpu.make_async_copy(x.at[span], encoded.at[span], out_sem.at[pair])

    def kept_copy(k):
        return pltpu.make_async_copy(
            a.at[k % 2, pl.ds(fr, cf), pl.ds(1, h), :, pl.ds(c, c)], kept.at[:, k], kept_sem.at[k]
        )

    def settle(k):
        wait_sent(True, k)
        wait_sent(False, k)
        for number in range(peers - 1):
            stat_copy(k, number, me).wait_send()

    load_x.wait()

    def widen(f, carry):
        sums, squares = carry
        values = x[f].astype(F32)
        v[f] = values
        slabs = values.reshape(h * w // 8, 8, c)
        return sums + jnp.sum(slabs, axis=0), squares + jnp.sum(slabs * slabs, axis=0)

    zero = jnp.zeros((8, c), F32)
    carry = lax.fori_loop(0, fr, widen, (zero, zero))
    pl.semaphore_wait(barrier, peers - 1)
    send_stats(0, *carry)
    for part in range(parts):
        send_halo(True, 0, part)

    def send_cached(k):
        def widen_cache(f, carry):
            vc[k, f] = cb[f, k].astype(F32)
            return carry

        lax.fori_loop(0, cf, widen_cache, 0)
        send_halo(False, k, 0)

    load_c.wait()
    send_cached(0)
    for k in range(convs):
        if k >= 2:
            kept_copy(k - 2).wait()
        wait_halo(False, k)
        build_cached(k)
        for copy in weight_copies(k):
            copy.wait()
        conv_cached(k)
        if k < convs - 1:
            for copy in weight_copies(k + 1):
                copy.start()
            send_cached(k + 1)
        if k:
            settle(k - 1)
        multiplier, offset = wait_stats(k)
        wait_halo(True, k)
        build_live(k, multiplier, offset)
        kept_copy(k).start()
        carry = conv_live(k)
        if k < convs - 1:
            send_stats(k + 1, *carry)
            send_halo(True, k + 1, parts - 1)

    settle(convs - 1)
    for k in range(max(convs - 2, 0), convs):
        kept_copy(k).wait()
    for pair in range(parts):
        out_copy(pair).wait()


def local(nh, nw, frames, caches, conv_weights, conv_bias, norm_gain, norm_shift):
    fr, h, w, c = frames.shape
    cf, convs = caches.shape[:2]
    dims = (nh, nw, fr, cf, convs, h, w, c)
    peers = nh * nw
    vmem = pltpu.VMEM
    dma = pltpu.SemaphoreType.DMA
    scratch = [
        vmem((fr, h * w, c), BF16),
        vmem((cf, convs, h * w, c), BF16),
        vmem((fr, h * w, c), F32),
        vmem((convs, cf, h * w, c), F32),
        vmem((2, fr + cf, h + 2, w, 3 * c), BF16),
        vmem((convs, 4, 3, 3 * c, 2 * c), BF16),
        vmem((h * w, 2 * c), F32),
        vmem(((h + 2) * (w + 8), c), F32),
        vmem((convs, 2, c), F32),
        vmem((convs, peers, 2, c), F32),
    ]
    for nf in (fr, cf):
        scratch += [
            vmem((convs, 2, nf, w, c), BF16),
            vmem((convs, 2, nf, h, c), BF16),
            vmem((convs, 4, nf, 1, c), F32),
            vmem((convs, 2, nf, w, c), BF16),
            vmem((convs, 2, nf, h, c), BF16),
            vmem((convs, 4, nf, 1, c), F32),
        ]
    scratch += [
        dma((2,)),
        dma((convs, 6)),
        dma((convs,)),
        dma((fr // 2,)),
        dma((convs, peers - 1)),
        dma((convs, peers)),
        dma((convs * (fr // 2 + 1), 8)),
        dma((convs * (fr // 2 + 1), 8)),
    ]
    anywhere = pl.BlockSpec(memory_space=pl.ANY)
    inside = pl.BlockSpec(memory_space=pltpu.VMEM)
    encoded, kept = pl.pallas_call(
        functools.partial(kernel, dims),
        out_shape=(
            jax.ShapeDtypeStruct((fr, h * w, c), BF16),
            jax.ShapeDtypeStruct(caches.shape, BF16),
        ),
        in_specs=[anywhere] * 3 + [inside] * 3,
        out_specs=(anywhere, anywhere),
        scratch_shapes=scratch,
        compiler_params=pltpu.CompilerParams(
            collective_id=0, has_side_effects=True, vmem_limit_bytes=56 * 1024 * 1024
        ),
    )(
        frames.reshape(fr, h * w, c),
        caches.reshape(cf, convs, h * w, c),
        conv_weights.reshape(convs, 3, 3, 3 * c, c),
        conv_bias,
        norm_gain,
        norm_shift,
    )
    return encoded.reshape(frames.shape), kept


def solution(mesh):
    return jax.shard_map(
        functools.partial(local, mesh.shape["ha"], mesh.shape["wa"]),
        mesh=mesh,
        in_specs=(
            P("clip", "ha", "wa", None),
            P("clip", None, "ha", "wa", None),
            P(),
            P(),
            P(),
            P(),
        ),
        out_specs=(P("clip", "ha", "wa", None), P("clip", None, "ha", "wa", None)),
        check_vma=False,
    )
```
